32 devices in a mesh: freq: 8 (over z, x), tm: 4 (over y, core).
Axes of the slice: x: 2, y: 2, z: 4, core: 2. Of those that a mesh axis runs over, the one named last changes fastest.
Arguments:
- vis: float32 [2, 32, 16, 1891], P(None, 'freq', 'tm'), may hold values from -12 to 12
- coherency: float32 [10, 2, 32, 16, 1891], P(None, None, 'freq', 'tm'), may hold values from -3 to 3
- pairs: int32 [2, 1891], replicated, may hold values from 0 to 61, as said below
- rho: float32 [10], replicated, may hold values from 30 to 300
- gains: float32 [2, 32, 10, 62], P(None, 'freq'), may hold values from -5 to 5
- duals: float32 [2, 32, 10, 62], P(None, 'freq'), may hold values from -50 to 50
- consensus: float32 [2, 4, 10, 62], replicated, may hold values from -5 to 5
Outputs:
- solved: float32 [2, 32, 10, 62], P(None, 'freq')
- duals_new: float32 [2, 32, 10, 62], P(None, 'freq')
- consensus_new: float32 [2, 4, 10, 62], replicated
The draws below stay inside these ranges and needn't reach their ends.
Inputs may be any that keep to these rules, and one draw needn't show every extreme that they name: `pairs`: every unordered pair of two different stations of 0 to 61 is one baseline, exactly once, in an arbitrary order and orientation.
All inputs are finite; a program needn't handle non-finite values.
Results may differ from the reference program's by a relative error of at most 0.0003.
Values sent between devices are 32-bit elements; how exact they have to be, the bound alone decides.
No kernel may reach another device: no remote copies, remote signals or barrier semaphores. Data moves between devices by JAX's collectives and lax.ppermute only.
A program may use at most 64 MiB of HBM per device.

```python
import math
import jax
import jax.numpy as jnp
import numpy as np
from jax import lax

STATIONS = 62
SKY_DIRECTIONS = 10
BASIS = 4
SWEEPS = 4
STATION_PAIRS = 1891
FREQ_CHANNELS = 32
TIME_SLOTS = 16


def draw_pairs(key, part):
    upper_rows, upper_cols = np.triu_indices(STATIONS, 1)
    ordering_key = jax.random.fold_in(key, 11)
    reversal_key = jax.random.fold_in(key, 12)
    pair_ordering = jax.random.permutation(ordering_key, STATION_PAIRS)
    reversed_pairs = jax.random.randint(reversal_key, (STATION_PAIRS,), 0, 2)
    lower_side = jnp.asarray(upper_rows, dtype=jnp.int32)[pair_ordering]
    upper_side = jnp.asarray(upper_cols, dtype=jnp.int32)[pair_ordering]
    first = jnp.where(reversed_pairs == 1, upper_side, lower_side)
    second = jnp.where(reversed_pairs == 1, lower_side, upper_side)
    return jnp.stack([first, second]).astype(jnp.int32)


def level_of(stream_key, extent, cuts, low, high):
    loudness, own = 1.0, jax.random.fold_in(stream_key, 6)
    for dim, blocks in cuts:
        heights = jnp.exp(jax.random.uniform(jax.random.fold_in(own, dim), (blocks,), jnp.float32, low / len(cuts), high / len(cuts)))
        loudness = loudness * jnp.repeat(heights, extent[dim] // blocks).reshape([-1 if axis == dim else 1 for axis in range(len(extent))])
    return loudness


def noise(rng, extent, width, reach, pieces=(), held_as=jnp.bfloat16):
    loudness = level_of(rng, extent, pieces, -0.22, 0.18) if pieces else 1.0
    values = jax.random.normal(rng, extent, jnp.float32) * width * loudness
    return jnp.minimum(jnp.maximum(values, -reach), reach).astype(held_as)


def setup_inputs(seed: int = 0) -> dict:
    streams_of = jax.random.split(jax.random.key(seed), 8)
    return {
        "vis": noise(streams_of[0], (2, FREQ_CHANNELS, TIME_SLOTS, STATION_PAIRS), 2.0, 12.0, ((1, 8), (2, 4)), jnp.float32),
        "coherency": noise(streams_of[1], (SKY_DIRECTIONS, 2, FREQ_CHANNELS, TIME_SLOTS, STATION_PAIRS), 0.5, 3.0, ((2, 8), (3, 4)), jnp.float32),
        "pairs": draw_pairs(jax.random.fold_in(streams_of[7], 71), 0),
        "rho": jnp.clip(jnp.exp(jax.random.uniform(streams_of[3], (SKY_DIRECTIONS,), jnp.float32, math.log(30.0), math.log(300.0))), 30.0, 300.0),
        "gains": noise(streams_of[4], (2, FREQ_CHANNELS, SKY_DIRECTIONS, STATIONS), 1.0, 5.0, ((1, 8),), jnp.float32),
        "duals": noise(streams_of[5], (2, FREQ_CHANNELS, SKY_DIRECTIONS, STATIONS), 10.0, 50.0, ((1, 8),), jnp.float32),
        "consensus": noise(streams_of[6], (2, BASIS, SKY_DIRECTIONS, STATIONS), 1.0, 5.0, (), jnp.float32),
    }


highest = lax.Precision.HIGHEST

def basis_rows(start, count, total):
    position = (start + jnp.arange(count, dtype=jnp.int32)).astype(jnp.float32)
    upper = (position + 0.5) / total
    lower = 1.0 - upper
    return jnp.stack([lower * lower * lower, 3.0 * upper * lower * lower, 3.0 * upper * upper * lower, upper * upper * upper])

def one_hot(station, count):
    return (station[:, None] == jnp.arange(count, dtype=jnp.int32)[None, :]).astype(jnp.float32)

def normal_terms(vis, coherency, gains, first, second):
    gain_first = jnp.einsum('rcks,bs->rkcb', gains, first, precision=highest)[:, :, :, None, :]
    gain_second = jnp.einsum('rcks,bs->rkcb', gains, second, precision=highest)[:, :, :, None, :]
    coh_real = coherency[:, 0]
    coh_imag = coherency[:, 1]
    lead_real = coh_real * gain_second[0] + coh_imag * gain_second[1]
    lead_imag = coh_imag * gain_second[0] - coh_real * gain_second[1]
    model_real = gain_first[0] * lead_real - gain_first[1] * lead_imag
    model_imag = gain_first[0] * lead_imag + gain_first[1] * lead_real
    error_real = vis[0] - jnp.sum(model_real, axis=0)
    error_imag = vis[1] - jnp.sum(model_imag, axis=0)
    resid_real = error_real[None] + model_real
    resid_imag = error_imag[None] + model_imag
    tail_real = coh_real * gain_first[0] - coh_imag * gain_first[1]
    tail_imag = coh_real * gain_first[1] + coh_imag * gain_first[0]
    first_real = jnp.sum(resid_real * lead_real + resid_imag * lead_imag, axis=2)
    first_imag = jnp.sum(resid_imag * lead_real - resid_real * lead_imag, axis=2)
    second_real = jnp.sum(resid_real * tail_real + resid_imag * tail_imag, axis=2)
    second_imag = jnp.sum(resid_real * tail_imag - resid_imag * tail_real, axis=2)
    first_power = jnp.sum(lead_real * lead_real + lead_imag * lead_imag, axis=2)
    second_power = jnp.sum(tail_real * tail_real + tail_imag * tail_imag, axis=2)

    def stations(by_first, by_second):
        return jnp.einsum('kcb,bs->cks', by_first, first, precision=highest) + jnp.einsum('kcb,bs->cks', by_second, second, precision=highest)
    return (stations(first_real, second_real), stations(first_imag, second_imag), stations(first_power, second_power))

def refine(gains, numer_real, numer_imag, power, target, rho):
    scale = power + rho[None, :, None]
    fresh = jnp.stack([(numer_real + target[0]) / scale, (numer_imag + target[1]) / scale])
    return 0.5 * (gains + fresh)

def fit_consensus(rhs, basis):
    gram = jnp.dot(basis, basis.T, precision=highest)
    factor = jnp.linalg.cholesky(gram)
    flat = jnp.moveaxis(rhs, 1, 0).reshape(rhs.shape[1], -1)
    solved = jax.scipy.linalg.cho_solve((factor, True), flat)
    return jnp.moveaxis(solved.reshape(rhs.shape[1], rhs.shape[0], rhs.shape[2], rhs.shape[3]), 0, 1)

def reference(vis, coherency, pairs, rho, gains, duals, consensus):
    total = vis.shape[1]
    basis = basis_rows(0, total, total)
    first = one_hot(pairs[0], STATIONS)
    second = one_hot(pairs[1], STATIONS)
    prior = jnp.einsum('mc,rmks->rcks', basis, consensus, precision=highest)
    target = rho[None, None, :, None] * prior - duals

    def per_channel(channel):
        vis_one = lax.dynamic_slice_in_dim(vis, channel, 1, 1)
        coh_one = lax.dynamic_slice_in_dim(coherency, channel, 1, 2)
        gains_one = lax.dynamic_slice_in_dim(gains, channel, 1, 1)
        target_one = lax.dynamic_slice_in_dim(target, channel, 1, 1)
        for sweep in range(SWEEPS):
            numer_real, numer_imag, power = normal_terms(vis_one, coh_one, gains_one, first, second)
            gains_one = refine(gains_one, numer_real, numer_imag, power, target_one, rho)
        return gains_one[:, 0]
    solved = jnp.moveaxis(lax.map(per_channel, jnp.arange(total, dtype=jnp.int32)), 0, 1)
    weighted = solved + duals / rho[None, None, :, None]
    rhs = jnp.einsum('mc,rcks->rmks', basis, weighted, precision=highest)
    consensus_new = fit_consensus(rhs, basis)
    prior_new = jnp.einsum('mc,rmks->rcks', basis, consensus_new, precision=highest)
    duals_new = duals + rho[None, None, :, None] * (solved - prior_new)
    return (solved, duals_new, consensus_new)
```

```python
import functools

import jax
import jax.numpy as jnp
import numpy as np
from jax import lax
from jax.experimental import pallas as pl
from jax.experimental.pallas import tpu as pltpu
from jax.sharding import PartitionSpec as P

SWEEPS = 4
LANES = 128
HALF = 64

highest = lax.Precision.HIGHEST


def basis_values(upper):
    lower = 1.0 - upper
    return (
        lower * lower * lower,
        3.0 * upper * lower * lower,
        3.0 * upper * upper * lower,
        upper * upper * upper,
    )


def gram_inverse(total):
    rows = np.stack(basis_values((np.arange(total) + 0.5) / total))
    return np.linalg.inv(rows @ rows.T)


def pick(index, values):
    out = values[-1]
    for m in range(len(values) - 2, -1, -1):
        out = jnp.where(index == m, values[m], out)
    return out


def evaluate(offset, rows, per, total, terms):
    row = lax.broadcasted_iota(jnp.int32, (rows, rows // per * terms), 0)
    col = lax.broadcasted_iota(jnp.int32, (rows, rows // per * terms), 1)
    upper = ((offset + row % per).astype(jnp.float32) + 0.5) / total
    value = pick(col % terms, basis_values(upper))
    return jnp.where(row // per == col // terms, value, 0.0)


def project(offset, rows, per, total, terms):
    row = lax.broadcasted_iota(jnp.int32, (rows // per * terms, rows), 0)
    col = lax.broadcasted_iota(jnp.int32, (rows // per * terms, rows), 1)
    upper = ((offset + col % per).astype(jnp.float32) + 0.5) / total
    values = basis_values(upper)
    inverse = gram_inverse(total)
    mixed = [
        functools.reduce(jnp.add, [float(inverse[m, n]) * values[n] for n in range(terms)])
        for m in range(terms)
    ]
    return jnp.where(row // terms == col // per, pick(row % terms, mixed), 0.0)


def rho_rows(rho_ref, rows, per):
    index = lax.broadcasted_iota(jnp.int32, (rows, LANES), 0) // per
    out = jnp.full((rows, LANES), rho_ref[0], jnp.float32)
    for k in range(1, rows // per):
        out = jnp.where(index == k, rho_ref[k], out)
    return out


def pack(native_ref, packed_ref, count):
    _, directions, per, _ = native_ref.shape
    packed_ref[...] = jnp.zeros(packed_ref.shape, jnp.float32)
    for k in range(directions):
        for r in range(2):
            packed_ref[k * per:(k + 1) * per, r * HALF:r * HALF + count] = native_ref[r, k]


def unpack(packed, scratch_ref, native_ref):
    _, directions, per, count = native_ref.shape
    scratch_ref[...] = packed
    for k in range(directions):
        for r in range(2):
            native_ref[r, k] = scratch_ref[k * per:(k + 1) * per, r * HALF:r * HALF + count]


def total_of(parts):
    while len(parts) > 1:
        parts = [parts[i] + parts[i + 1] for i in range(0, len(parts), 2)]
    return parts[0]


def split_rows(rows):
    return -(-(rows // 2) // 8) * 8


def refine(sums, gains, target, rho):
    rows = gains.shape[0]
    top = split_rows(rows)
    numer = sums[:rows]
    tail = sums[rows:]
    power = jnp.concatenate([tail[:, :HALF], tail[:rows - top, HALF:]], axis=0)
    power = jnp.concatenate([power, power], axis=1)
    return 0.5 * (gains + (numer + target) / (power + rho))


def gather_rows(gains):
    rows = jnp.concatenate([gains[:, :HALF], gains[:, HALF:]], axis=0)
    high = rows.astype(jnp.bfloat16).astype(jnp.float32)
    return jnp.concatenate([high, rows - high], axis=1).astype(jnp.bfloat16)


def hot(pairs_row):
    index = lax.broadcasted_iota(jnp.int32, (LANES, pairs_row.shape[1]), 0) % HALF
    return jnp.where(index == pairs_row, 1.0, 0.0).astype(jnp.bfloat16)


def places(rows, times):
    power = 2 * times * rows
    seen = power + rows
    height = max(seen + 2 * times * 8, times * rows + 8 * rows, seen + times * 8 + 64)
    return power, seen, -(-height // 8) * 8


def sweep_tile(j, per, times, tile_ref, at_ref, by_first, by_second):
    rows = at_ref.shape[1] // 4
    pow_at, vis_at, _ = places(rows, times)
    groups = rows // 8

    def gained(i):
        return at_ref[j, i * rows:(i + 1) * rows, :].reshape(groups, 8, LANES)

    p_real, p_imag, q_real, q_imag = [gained(i) for i in range(4)]
    m_real = p_real * q_real + p_imag * q_imag
    m_imag = p_imag * q_real - p_real * q_imag
    weight = tile_ref[j, pow_at:pow_at + rows, :].reshape(groups, 8, LANES)
    s_real = m_real * weight
    s_imag = m_imag * weight

    def over_directions(x):
        x = jnp.sum(x, axis=0)
        shift = per
        while shift < 8:
            x = x + pltpu.roll(x, shift, 0)
            shift *= 2
        return x

    for t in range(times):
        c_real = tile_ref[j, t * rows:(t + 1) * rows, :].reshape(groups, 8, LANES)
        c_imag = tile_ref[j, (times + t) * rows:(times + t + 1) * rows, :].reshape(groups, 8, LANES)
        e_real = tile_ref[j, vis_at + t * 8:vis_at + t * 8 + 8, :] - over_directions(m_real * c_real - m_imag * c_imag)
        e_imag = tile_ref[j, vis_at + (times + t) * 8:vis_at + (times + t) * 8 + 8, :] - over_directions(m_real * c_imag + m_imag * c_real)
        s_real = s_real + (e_real * c_real + e_imag * c_imag)
        s_imag = s_imag + (e_imag * c_real - e_real * c_imag)

    def put(ref, real, imag, power):
        stack = jnp.concatenate([x.reshape(rows, LANES) for x in (real, imag, power)], axis=0)
        high = stack.astype(jnp.bfloat16).astype(jnp.float32)
        ref[j] = jnp.concatenate([high, stack - high], axis=0).astype(jnp.bfloat16)

    put(
        by_first,
        s_real * q_real - s_imag * q_imag,
        s_real * q_imag + s_imag * q_real,
        weight * (q_real * q_real + q_imag * q_imag),
    )
    put(
        by_second,
        s_real * p_real + s_imag * p_imag,
        s_real * p_imag - s_imag * p_real,
        weight * (p_real * p_real + p_imag * p_imag),
    )


def sweep_block(gains, pairs_ref, tiles, per, times, tile_ref, at_ref, by_first, by_second):
    rows = gains.shape[0]
    left = gather_rows(gains)
    pairs = pairs_ref[...]
    first = hot(pairs[0:1])
    second = hot(pairs[1:2])
    for side, choice in enumerate((first, second)):
        at_all = jnp.dot(left, choice, preferred_element_type=jnp.float32)
        for j in range(tiles):
            at_ref[j, side * 2 * rows:(side + 1) * 2 * rows, :] = at_all[:, j * LANES:(j + 1) * LANES]

    def step(j, carry):
        sweep_tile(j, per, times, tile_ref, at_ref, by_first, by_second)
        return carry

    lax.fori_loop(0, tiles, step, 0)
    across = (((1,), (1,)), ((), ()))
    sums = 0.0
    for ref, choice in ((by_first, first), (by_second, second)):
        laid = jnp.concatenate([ref[j] for j in range(tiles)], axis=1)
        sums = sums + lax.dot_general(laid, choice[:HALF], across, preferred_element_type=jnp.float32)
    return sums[:3 * rows] + sums[3 * rows:]


def join(sums, rows):
    top = split_rows(rows)
    power = sums[2 * rows:]
    low = jnp.concatenate([power[top:], jnp.zeros((2 * top - rows, HALF), jnp.float32)], axis=0)
    return jnp.concatenate(
        [
            jnp.concatenate([sums[:rows], sums[rows:2 * rows]], axis=1),
            jnp.concatenate([power[:top], low], axis=1),
        ],
        axis=0,
    )


def opening_kernel(
    sizes, offset_ref, rho_ref, coh_in, vis_in, pairs_ref, gains_in, duals_in, cons_in,
    tile_ref, gains_ref, target_ref, sums_ref,
    acc_ref, pad_ref, at_ref, by_first, by_second,
):
    per, times, total, count, pairs_count, tiles = sizes
    directions = coh_in.shape[0]
    rows = directions * per
    pow_at, vis_at, _ = places(rows, times)
    step = pl.program_id(0)

    @pl.when(step == 0)
    def _():
        pack(gains_in, gains_ref, count)
        pack(cons_in, pad_ref, count)
        terms = cons_in.shape[2]
        prior = jnp.dot(
            evaluate(offset_ref[0], rows, per, total, terms), pad_ref[...],
            precision=highest, preferred_element_type=jnp.float32,
        )
        pack(duals_in, target_ref, count)
        target_ref[...] = rho_rows(rho_ref, rows, per) * prior - target_ref[...]
        acc_ref[...] = jnp.zeros(acc_ref.shape, jnp.float32)

    for j in range(tiles):
        lanes = slice(j * LANES, (j + 1) * LANES)
        place = (step * tiles + j) * LANES + lax.broadcasted_iota(jnp.int32, (times, LANES), 1)
        keep = place < pairs_count
        for r in range(2):
            for c in range(per):
                block = jnp.where(keep, vis_in[r, c, :, lanes], 0.0)
                for copy in range(8 // per):
                    tile_ref[j, pl.ds(vis_at + r * times * 8 + copy * per + c, times, stride=8), :] = block
                for k in range(directions):
                    tile_ref[j, pl.ds(r * times * rows + k * per + c, times, stride=rows), :] = jnp.where(
                        keep, coh_in[k, r, c, :, lanes], 0.0
                    )
        power = jnp.zeros((rows, LANES), jnp.float32)
        for t in range(2 * times):
            c_part = tile_ref[j, t * rows:(t + 1) * rows, :]
            power = power + c_part * c_part
        tile_ref[j, pow_at:pow_at + rows, :] = power

    acc_ref[...] += sweep_block(
        gains_ref[...], pairs_ref, tiles, per, times, tile_ref, at_ref, by_first, by_second
    )

    @pl.when(step == pl.num_programs(0) - 1)
    def _():
        sums_ref[...] = join(acc_ref[...], rows)


def sweep_kernel(sizes, ways, rho_ref, *refs):
    per, times, total, count, pairs_count, tiles = sizes
    parts = refs[:ways]
    gains_in, target_ref, tile_ref, pairs_ref, gains_ref, sums_ref = refs[ways:ways + 6]
    at_ref, by_first, by_second = refs[ways + 6:]
    rows = gains_in.shape[0]
    gains = refine(
        total_of([part[...] for part in parts]), gains_in[...], target_ref[...], rho_rows(rho_ref, rows, per)
    )
    gains_ref[...] = gains
    sums_ref[...] = join(
        sweep_block(
            gains, pairs_ref, tile_ref.shape[0], per, times, tile_ref, at_ref, by_first, by_second
        ),
        rows,
    )


def closing_kernel(sizes, terms, ways, offset_ref, rho_ref, *refs):
    per, times, total, count, pairs_count, tiles = sizes
    parts = refs[:ways]
    gains_in, target_ref, duals_in, gains_ref, solved_ref, fit_ref, pad_ref = refs[ways:]
    rows = gains_in.shape[0]
    rho = rho_rows(rho_ref, rows, per)
    gains = refine(total_of([part[...] for part in parts]), gains_in[...], target_ref[...], rho)
    pack(duals_in, pad_ref, count)
    weighted = gains + pad_ref[...] / rho
    fit_ref[...] = jnp.dot(
        project(offset_ref[0], rows, per, total, terms), weighted,
        precision=highest, preferred_element_type=jnp.float32,
    )
    gains_ref[...] = gains
    unpack(gains, pad_ref, solved_ref)


def final_kernel(sizes, ways, offset_ref, rho_ref, *refs):
    per, times, total, count, pairs_count, tiles = sizes
    parts = refs[:ways]
    gains_ref, duals_in, duals_ref, cons_ref, pad_ref, cons_pad = refs[ways:]
    rows = gains_ref.shape[0]
    terms = cons_ref.shape[2]
    cons = total_of([part[...] for part in parts])
    prior = jnp.dot(
        evaluate(offset_ref[0], rows, per, total, terms), cons,
        precision=highest, preferred_element_type=jnp.float32,
    )
    pack(duals_in, pad_ref, count)
    fresh = pad_ref[...] + rho_rows(rho_ref, rows, per) * (gains_ref[...] - prior)
    unpack(fresh, pad_ref, duals_ref)
    unpack(cons, cons_pad, cons_ref)


def exchange(x, axis, strides):
    count = lax.axis_size(axis)
    return [x] + [lax.ppermute(x, axis, [(i, i ^ s) for i in range(count)]) for s in strides]


def shape_of(*dims, dtype=jnp.float32):
    return jax.ShapeDtypeStruct(dims, dtype)


vmem = pl.BlockSpec(memory_space=pltpu.VMEM)
smem = pl.BlockSpec(memory_space=pltpu.SMEM)


def local(vis, coherency, pairs, rho, gains, duals, consensus):
    directions, _, per, times, pairs_count = coherency.shape
    count = gains.shape[3]
    terms = consensus.shape[1]
    rows = directions * per
    total = per * lax.axis_size("freq")
    offset = (lax.axis_index("freq") * per).astype(jnp.int32).reshape(1)
    all_tiles = -(-pairs_count // LANES)
    tiles = max(d for d in range(1, 6) if all_tiles % d == 0)
    steps = all_tiles // tiles
    width = tiles * LANES
    pairs = jnp.pad(pairs, ((0, 8 - pairs.shape[0]), (0, all_tiles * LANES - pairs_count)), constant_values=-1)
    gains = jnp.swapaxes(gains, 1, 2)
    duals = jnp.swapaxes(duals, 1, 2)
    consensus = jnp.swapaxes(consensus, 1, 2)
    sizes = (per, times, total, count, pairs_count, tiles)
    sum_rows = rows + split_rows(rows)
    height = places(rows, times)[2]
    packed = shape_of(rows, LANES)

    def work(blocks):
        return [
            pltpu.VMEM((blocks, 4 * rows, LANES), jnp.float32),
            pltpu.VMEM((blocks, 6 * rows, LANES), jnp.bfloat16),
            pltpu.VMEM((blocks, 6 * rows, LANES), jnp.bfloat16),
        ]

    tile_data, gains_now, target, sums = pl.pallas_call(
        functools.partial(opening_kernel, sizes),
        name="opening",
        grid=(steps,),
        in_specs=[
            smem,
            smem,
            pl.BlockSpec((directions, 2, per, times, width), lambda i: (0, 0, 0, 0, i)),
            pl.BlockSpec((2, per, times, width), lambda i: (0, 0, 0, i)),
            pl.BlockSpec((8, width), lambda i: (0, i)),
            pl.BlockSpec(gains.shape, lambda i: (0, 0, 0, 0)),
            pl.BlockSpec(duals.shape, lambda i: (0, 0, 0, 0)),
            pl.BlockSpec(consensus.shape, lambda i: (0, 0, 0, 0)),
        ],
        out_specs=[
            pl.BlockSpec((tiles, height, LANES), lambda i: (i, 0, 0)),
            pl.BlockSpec((rows, LANES), lambda i: (0, 0)),
            pl.BlockSpec((rows, LANES), lambda i: (0, 0)),
            pl.BlockSpec((sum_rows, LANES), lambda i: (0, 0)),
        ],
        out_shape=[
            shape_of(all_tiles, height, LANES),
            packed,
            packed,
            shape_of(sum_rows, LANES),
        ],
        scratch_shapes=[
            pltpu.VMEM((3 * rows, HALF), jnp.float32),
            pltpu.VMEM((rows, LANES), jnp.float32),
        ] + work(tiles),
    )(offset, rho, coherency, vis, pairs, gains, duals, consensus)

    ways = lax.axis_size("tm")
    peers = range(1, ways)
    for _ in range(SWEEPS - 1):
        gains_now, sums = pl.pallas_call(
            functools.partial(sweep_kernel, sizes, ways),
            name="sweep",
            in_specs=[smem] + [vmem] * (ways + 4),
            out_specs=[vmem, vmem],
            out_shape=[packed, shape_of(sum_rows, LANES)],
            scratch_shapes=work(all_tiles),
        )(rho, *exchange(sums, "tm", peers), gains_now, target, tile_data, pairs)

    gains_now, solved, fit = pl.pallas_call(
        functools.partial(closing_kernel, sizes, terms, ways),
        name="closing",
        in_specs=[smem, smem] + [vmem] * (ways + 3),
        out_specs=[vmem] * 3,
        out_shape=[packed, shape_of(2, directions, per, count), shape_of(directions * terms, LANES)],
        scratch_shapes=[pltpu.VMEM((rows, LANES), jnp.float32)],
    )(offset, rho, *exchange(sums, "tm", peers), gains_now, target, duals)

    span = lax.axis_size("freq")
    stride = 1
    while stride * 4 < span:
        fit = total_of(exchange(fit, "freq", [stride, 2 * stride, 3 * stride]))
        stride *= 4
    parts = exchange(fit, "freq", range(stride, span, stride))
    duals_new, consensus_new = pl.pallas_call(
        functools.partial(final_kernel, sizes, len(parts)),
        name="final",
        in_specs=[smem, smem] + [vmem] * (len(parts) + 2),
        out_specs=[vmem] * 2,
        out_shape=[shape_of(2, directions, per, count), shape_of(2, directions, terms, count)],
        scratch_shapes=[
            pltpu.VMEM((rows, LANES), jnp.float32),
            pltpu.VMEM((directions * terms, LANES), jnp.float32),
        ],
    )(offset, rho, *parts, gains_now, duals)
    return tuple(jnp.swapaxes(x, 1, 2) for x in (solved, duals_new, consensus_new))


def solution(mesh):
    in_specs = (
        P(None, "freq", "tm", None),
        P(None, None, "freq", "tm", None),
        P(),
        P(),
        P(None, "freq", None, None),
        P(None, "freq", None, None),
        P(),
    )
    out_specs = (P(None, "freq", None, None), P(None, "freq", None, None), P())
    return jax.shard_map(local, mesh=mesh, in_specs=in_specs, out_specs=out_specs, check_vma=False)
```

```python
import functools

import jax
import jax.numpy as jnp
import numpy as np
from jax import lax
from jax.experimental import pallas as pl
from jax.experimental.pallas import tpu as pltpu
from jax.sharding import PartitionSpec as P

SWEEPS = 4
LANES = 128
HALF = 64

highest = lax.Precision.HIGHEST


def basis_values(upper):
    lower = 1.0 - upper
    return (
        lower * lower * lower,
        3.0 * upper * lower * lower,
        3.0 * upper * upper * lower,
        upper * upper * upper,
    )


def gram_inverse(total):
    rows = np.stack(basis_values((np.arange(total) + 0.5) / total))
    return np.linalg.inv(rows @ rows.T)


def pick(index, values):
    out = values[-1]
    for m in range(len(values) - 2, -1, -1):
        out = jnp.where(index == m, values[m], out)
    return out


def evaluate(offset, rows, per, total, terms):
    row = lax.broadcasted_iota(jnp.int32, (rows, rows // per * terms), 0)
    col = lax.broadcasted_iota(jnp.int32, (rows, rows // per * terms), 1)
    upper = ((offset + row % per).astype(jnp.float32) + 0.5) / total
    value = pick(col % terms, basis_values(upper))
    return jnp.where(row // per == col // terms, value, 0.0)


def project(offset, rows, per, total, terms):
    row = lax.broadcasted_iota(jnp.int32, (rows // per * terms, rows), 0)
    col = lax.broadcasted_iota(jnp.int32, (rows // per * terms, rows), 1)
    upper = ((offset + col % per).astype(jnp.float32) + 0.5) / total
    values = basis_values(upper)
    inverse = gram_inverse(total)
    mixed = [
        functools.reduce(jnp.add, [float(inverse[m, n]) * values[n] for n in range(terms)])
        for m in range(terms)
    ]
    return jnp.where(row // terms == col // per, pick(row % terms, mixed), 0.0)


def rho_rows(rho_ref, rows, per):
    index = lax.broadcasted_iota(jnp.int32, (rows, LANES), 0) // per
    out = jnp.full((rows, LANES), rho_ref[0], jnp.float32)
    for k in range(1, rows // per):
        out = jnp.where(index == k, rho_ref[k], out)
    return out


def pack(native_ref, packed_ref, count):
    _, directions, per, _ = native_ref.shape
    packed_ref[...] = jnp.zeros(packed_ref.shape, jnp.float32)
    for k in range(directions):
        for r in range(2):
            packed_ref[k * per:(k + 1) * per, r * HALF:r * HALF + count] = native_ref[r, k]


def unpack(packed, scratch_ref, native_ref):
    _, directions, per, count = native_ref.shape
    scratch_ref[...] = packed
    for k in range(directions):
        for r in range(2):
            native_ref[r, k] = scratch_ref[k * per:(k + 1) * per, r * HALF:r * HALF + count]


def total_of(parts):
    while len(parts) > 1:
        parts = [parts[i] + parts[i + 1] for i in range(0, len(parts), 2)]
    return parts[0]


def split_rows(rows):
    return -(-(rows // 2) // 8) * 8


def refine(sums, gains, target, rho):
    rows = gains.shape[0]
    top = split_rows(rows)
    numer = sums[:rows]
    tail = sums[rows:]
    power = jnp.concatenate([tail[:, :HALF], tail[:rows - top, HALF:]], axis=0)
    power = jnp.concatenate([power, power], axis=1)
    return 0.5 * (gains + (numer + target) / (power + rho))


def gather_rows(gains):
    rows = jnp.concatenate([gains[:, :HALF], gains[:, HALF:]], axis=0)
    high = rows.astype(jnp.bfloat16).astype(jnp.float32)
    return jnp.concatenate([high, rows - high], axis=1).astype(jnp.bfloat16)


def hot(pairs_row):
    index = lax.broadcasted_iota(jnp.int32, (LANES, pairs_row.shape[1]), 0) % HALF
    return jnp.where(index == pairs_row, 1.0, 0.0).astype(jnp.bfloat16)


def places(rows, times):
    power = 2 * times * rows
    seen = power + rows
    height = max(seen + 2 * times * 8, times * rows + 8 * rows, seen + times * 8 + 64)
    return power, seen, -(-height // 8) * 8


def sweep_tile(j, per, times, tile_ref, at_ref, by_first, by_second):
    rows = at_ref.shape[1] // 4
    pow_at, vis_at, _ = places(rows, times)
    groups = rows // 8

    def gained(i):
        return at_ref[j, i * rows:(i + 1) * rows, :].reshape(groups, 8, LANES)

    p_real, p_imag, q_real, q_imag = [gained(i) for i in range(4)]
    m_real = p_real * q_real + p_imag * q_imag
    m_imag = p_imag * q_real - p_real * q_imag
    weight = tile_ref[j, pow_at:pow_at + rows, :].reshape(groups, 8, LANES)
    s_real = m_real * weight
    s_imag = m_imag * weight

    def over_directions(x):
        x = jnp.sum(x, axis=0)
        shift = per
        while shift < 8:
            x = x + pltpu.roll(x, shift, 0)
            shift *= 2
        return x

    for t in range(times):
        c_real = tile_ref[j, t * rows:(t + 1) * rows, :].reshape(groups, 8, LANES)
        c_imag = tile_ref[j, (times + t) * rows:(times + t + 1) * rows, :].reshape(groups, 8, LANES)
        e_real = tile_ref[j, vis_at + t * 8:vis_at + t * 8 + 8, :] - over_directions(m_real * c_real - m_imag * c_imag)
        e_imag = tile_ref[j, vis_at + (times + t) * 8:vis_at + (times + t) * 8 + 8, :] - over_directions(m_real * c_imag + m_imag * c_real)
        s_real = s_real + (e_real * c_real + e_imag * c_imag)
        s_imag = s_imag + (e_imag * c_real - e_real * c_imag)

    def put(ref, real, imag, power):
        stack = jnp.concatenate([x.reshape(rows, LANES) for x in (real, imag, power)], axis=0)
        high = stack.astype(jnp.bfloat16).astype(jnp.float32)
        ref[j] = jnp.concatenate([high, stack - high], axis=0).astype(jnp.bfloat16)

    put(
        by_first,
        s_real * q_real - s_imag * q_imag,
        s_real * q_imag + s_imag * q_real,
        weight * (q_real * q_real + q_imag * q_imag),
    )
    put(
        by_second,
        s_real * p_real + s_imag * p_imag,
        s_real * p_imag - s_imag * p_real,
        weight * (p_real * p_real + p_imag * p_imag),
    )


def sweep_block(gains, pairs_ref, tiles, per, times, tile_ref, at_ref, by_first, by_second, waits=()):
    rows = gains.shape[0]
    left = gather_rows(gains)
    pairs = pairs_ref[...]
    first = hot(pairs[0:1])
    second = hot(pairs[1:2])
    for side, choice in enumerate((first, second)):
        at_all = jnp.dot(left, choice, preferred_element_type=jnp.float32)
        for j in range(tiles):
            at_ref[j, side * 2 * rows:(side + 1) * 2 * rows, :] = at_all[:, j * LANES:(j + 1) * LANES]

    def step(j, carry):
        sweep_tile(j, per, times, tile_ref, at_ref, by_first, by_second)
        return carry

    blocks = max(len(waits), 1)
    for b in range(blocks):
        if waits:
            waits[b].wait()
        lax.fori_loop(b * tiles // blocks, (b + 1) * tiles // blocks, step, 0, unroll=True)
    across = (((1,), (1,)), ((), ()))
    sums = 0.0
    for ref, choice in ((by_first, first), (by_second, second)):
        laid = jnp.concatenate([ref[j] for j in range(tiles)], axis=1)
        sums = sums + lax.dot_general(laid, choice[:HALF], across, preferred_element_type=jnp.float32)
    return sums[:3 * rows] + sums[3 * rows:]


def join(sums, rows):
    top = split_rows(rows)
    power = sums[2 * rows:]
    low = jnp.concatenate([power[top:], jnp.zeros((2 * top - rows, HALF), jnp.float32)], axis=0)
    return jnp.concatenate(
        [
            jnp.concatenate([sums[:rows], sums[rows:2 * rows]], axis=1),
            jnp.concatenate([power[:top], low], axis=1),
        ],
        axis=0,
    )


def opening_kernel(
    sizes, offset_ref, rho_ref, coh_in, vis_in, pairs_in, gains_in, duals_in, cons_in,
    tile_ref, pairs_ref, gains_ref, target_ref, sums_ref,
    acc_ref, pad_ref, at_ref, by_first, by_second,
):
    per, times, total, count, pairs_count, tiles = sizes
    directions = coh_in.shape[0]
    rows = directions * per
    pow_at, vis_at, _ = places(rows, times)
    step = pl.program_id(0)

    @pl.when(step == 0)
    def _():
        pack(gains_in, gains_ref, count)
        pack(cons_in, pad_ref, count)
        terms = cons_in.shape[2]
        prior = jnp.dot(
            evaluate(offset_ref[0], rows, per, total, terms), pad_ref[...],
            precision=highest, preferred_element_type=jnp.float32,
        )
        pack(duals_in, target_ref, count)
        target_ref[...] = rho_rows(rho_ref, rows, per) * prior - target_ref[...]
        acc_ref[...] = jnp.zeros(acc_ref.shape, jnp.float32)

    width = tiles * LANES
    inside = step * width + lax.broadcasted_iota(jnp.int32, (2, width), 1) < pairs_count
    pairs_ref[0:2, :] = jnp.where(inside, pairs_in[...], -1)
    pairs_ref[2:8, :] = jnp.full((6, width), -1, jnp.int32)
    for j in range(tiles):
        lanes = slice(j * LANES, (j + 1) * LANES)
        place = (step * tiles + j) * LANES + lax.broadcasted_iota(jnp.int32, (times, LANES), 1)
        keep = place < pairs_count
        for r in range(2):
            for c in range(per):
                block = jnp.where(keep, vis_in[r, c, :, lanes], 0.0)
                for copy in range(8 // per):
                    tile_ref[j, pl.ds(vis_at + r * times * 8 + copy * per + c, times, stride=8), :] = block
                for k in range(directions):
                    tile_ref[j, pl.ds(r * times * rows + k * per + c, times, stride=rows), :] = jnp.where(
                        keep, coh_in[k, r, c, :, lanes], 0.0
                    )
        power = jnp.zeros((rows, LANES), jnp.float32)
        for t in range(2 * times):
            c_part = tile_ref[j, t * rows:(t + 1) * rows, :]
            power = power + c_part * c_part
        tile_ref[j, pow_at:pow_at + rows, :] = power

    acc_ref[...] += sweep_block(
        gains_ref[...], pairs_ref, tiles, per, times, tile_ref, at_ref, by_first, by_second
    )

    @pl.when(step == pl.num_programs(0) - 1)
    def _():
        sums_ref[...] = join(acc_ref[...], rows)


def sweep_kernel(sizes, ways, rho_ref, *refs):
    per, times, total, count, pairs_count, tiles = sizes
    parts = refs[:ways]
    gains_in, target_ref, tile_any, pairs_ref, gains_ref, sums_ref = refs[ways:ways + 6]
    tile_ref, arrived, at_ref, by_first, by_second = refs[ways + 6:]
    rows = gains_in.shape[0]
    all_tiles = tile_ref.shape[0]
    copies = [
        pltpu.make_async_copy(
            tile_any.at[pl.ds(b * tiles, tiles)], tile_ref.at[pl.ds(b * tiles, tiles)], arrived.at[b]
        )
        for b in range(all_tiles // tiles)
    ]
    for copy in copies:
        copy.start()
    gains = refine(
        total_of([part[...] for part in parts]), gains_in[...], target_ref[...], rho_rows(rho_ref, rows, per)
    )
    gains_ref[...] = gains
    sums = sweep_block(
        gains, pairs_ref, all_tiles, per, times, tile_ref, at_ref, by_first, by_second, copies
    )
    sums_ref[...] = join(sums, rows)


def closing_kernel(sizes, terms, ways, offset_ref, rho_ref, *refs):
    per, times, total, count, pairs_count, tiles = sizes
    parts = refs[:ways]
    gains_in, target_ref, duals_in, gains_ref, solved_ref, fit_ref, pad_ref = refs[ways:]
    rows = gains_in.shape[0]
    rho = rho_rows(rho_ref, rows, per)
    gains = refine(total_of([part[...] for part in parts]), gains_in[...], target_ref[...], rho)
    pack(duals_in, pad_ref, count)
    weighted = gains + pad_ref[...] / rho
    fit_ref[...] = jnp.dot(
        project(offset_ref[0], rows, per, total, terms), weighted,
        precision=highest, preferred_element_type=jnp.float32,
    )
    gains_ref[...] = gains
    unpack(gains, pad_ref, solved_ref)


def final_kernel(sizes, ways, offset_ref, rho_ref, *refs):
    per, times, total, count, pairs_count, tiles = sizes
    parts = refs[:ways]
    gains_ref, duals_in, duals_ref, cons_ref, pad_ref, cons_pad = refs[ways:]
    rows = gains_ref.shape[0]
    terms = cons_ref.shape[2]
    cons = total_of([part[...] for part in parts])
    prior = jnp.dot(
        evaluate(offset_ref[0], rows, per, total, terms), cons,
        precision=highest, preferred_element_type=jnp.float32,
    )
    pack(duals_in, pad_ref, count)
    fresh = pad_ref[...] + rho_rows(rho_ref, rows, per) * (gains_ref[...] - prior)
    unpack(fresh, pad_ref, duals_ref)
    unpack(cons, cons_pad, cons_ref)


def exchange(x, axis, strides):
    count = lax.axis_size(axis)
    return [x] + [lax.ppermute(x, axis, [(i, i ^ s) for i in range(count)]) for s in strides]


def shape_of(*dims, dtype=jnp.float32):
    return jax.ShapeDtypeStruct(dims, dtype)


vmem = pl.BlockSpec(memory_space=pltpu.VMEM)
smem = pl.BlockSpec(memory_space=pltpu.SMEM)


def local(vis, coherency, pairs, rho, gains, duals, consensus):
    directions, _, per, times, pairs_count = coherency.shape
    count = gains.shape[3]
    terms = consensus.shape[1]
    rows = directions * per
    total = per * lax.axis_size("freq")
    offset = (lax.axis_index("freq") * per).astype(jnp.int32).reshape(1)
    all_tiles = -(-pairs_count // LANES)
    tiles = max(d for d in range(1, 6) if all_tiles % d == 0)
    steps = all_tiles // tiles
    width = tiles * LANES
    gains = jnp.swapaxes(gains, 1, 2)
    duals = jnp.swapaxes(duals, 1, 2)
    consensus = jnp.swapaxes(consensus, 1, 2)
    sizes = (per, times, total, count, pairs_count, tiles)
    sum_rows = rows + split_rows(rows)
    height = places(rows, times)[2]
    packed = shape_of(rows, LANES)

    def work(blocks):
        return [
            pltpu.VMEM((blocks, 4 * rows, LANES), jnp.float32),
            pltpu.VMEM((blocks, 6 * rows, LANES), jnp.bfloat16),
            pltpu.VMEM((blocks, 6 * rows, LANES), jnp.bfloat16),
        ]

    tile_data, marked, gains_now, target, sums = pl.pallas_call(
        functools.partial(opening_kernel, sizes),
        name="opening",
        grid=(steps,),
        in_specs=[
            smem,
            smem,
            pl.BlockSpec((directions, 2, per, times, width), lambda i: (0, 0, 0, 0, i)),
            pl.BlockSpec((2, per, times, width), lambda i: (0, 0, 0, i)),
            pl.BlockSpec((2, width), lambda i: (0, i)),
            pl.BlockSpec(gains.shape, lambda i: (0, 0, 0, 0)),
            pl.BlockSpec(duals.shape, lambda i: (0, 0, 0, 0)),
            pl.BlockSpec(consensus.shape, lambda i: (0, 0, 0, 0)),
        ],
        out_specs=[
            pl.BlockSpec((tiles, height, LANES), lambda i: (i, 0, 0)),
            pl.BlockSpec((8, width), lambda i: (0, i)),
            pl.BlockSpec((rows, LANES), lambda i: (0, 0)),
            pl.BlockSpec((rows, LANES), lambda i: (0, 0)),
            pl.BlockSpec((sum_rows, LANES), lambda i: (0, 0)),
        ],
        out_shape=[
            shape_of(all_tiles, height, LANES),
            shape_of(8, all_tiles * LANES, dtype=jnp.int32),
            packed,
            packed,
            shape_of(sum_rows, LANES),
        ],
        scratch_shapes=[
            pltpu.VMEM((3 * rows, HALF), jnp.float32),
            pltpu.VMEM((rows, LANES), jnp.float32),
        ] + work(tiles),
    )(offset, rho, coherency, vis, pairs, gains, duals, consensus)

    ways = lax.axis_size("tm")
    peers = range(1, ways)
    for _ in range(SWEEPS - 1):
        gains_now, sums = pl.pallas_call(
            functools.partial(sweep_kernel, sizes, ways),
            name="sweep",
            in_specs=[smem] + [vmem] * (ways + 2) + [pl.BlockSpec(memory_space=pl.ANY), vmem],
            out_specs=[vmem, vmem],
            out_shape=[packed, shape_of(sum_rows, LANES)],
            scratch_shapes=[
                pltpu.VMEM((all_tiles, height, LANES), jnp.float32),
                pltpu.SemaphoreType.DMA((steps,)),
            ]
            + work(all_tiles),
        )(rho, *exchange(sums, "tm", peers), gains_now, target, tile_data, marked)

    gains_now, solved, fit = pl.pallas_call(
        functools.partial(closing_kernel, sizes, terms, ways),
        name="closing",
        in_specs=[smem, smem] + [vmem] * (ways + 3),
        out_specs=[vmem] * 3,
        out_shape=[packed, shape_of(2, directions, per, count), shape_of(directions * terms, LANES)],
        scratch_shapes=[pltpu.VMEM((rows, LANES), jnp.float32)],
    )(offset, rho, *exchange(sums, "tm", peers), gains_now, target, duals)

    span = lax.axis_size("freq")
    stride = 1
    while stride * 4 < span:
        fit = total_of(exchange(fit, "freq", [stride, 2 * stride, 3 * stride]))
        stride *= 4
    parts = exchange(fit, "freq", range(stride, span, stride))
    duals_new, consensus_new = pl.pallas_call(
        functools.partial(final_kernel, sizes, len(parts)),
        name="final",
        in_specs=[smem, smem] + [vmem] * (len(parts) + 2),
        out_specs=[vmem] * 2,
        out_shape=[shape_of(2, directions, per, count), shape_of(2, directions, terms, count)],
        scratch_shapes=[
            pltpu.VMEM((rows, LANES), jnp.float32),
            pltpu.VMEM((directions * terms, LANES), jnp.float32),
        ],
    )(offset, rho, *parts, gains_now, duals)
    return tuple(jnp.swapaxes(x, 1, 2) for x in (solved, duals_new, consensus_new))


def solution(mesh):
    in_specs = (
        P(None, "freq", "tm", None),
        P(None, None, "freq", "tm", None),
        P(),
        P(),
        P(None, "freq", None, None),
        P(None, "freq", None, None),
        P(),
    )
    out_specs = (P(None, "freq", None, None), P(None, "freq", None, None), P())
    return jax.shard_map(local, mesh=mesh, in_specs=in_specs, out_specs=out_specs, check_vma=False)
```
